8 devices in a mesh: dp: 1 (over z), tp: 8 (over x, y, core).
Axes of the slice: x: 2, y: 2, z: 1, core: 2. Of those that a mesh axis runs over, the one named last changes fastest.
Arguments:
- x: bfloat16 [2048, 5120], P('dp')
- w_gate: bfloat16 [5120, 16384], P(None, 'tp')
- w_up: bfloat16 [5120, 16384], P(None, 'tp')
- w_down: bfloat16 [16384, 5120], P('tp')
Outputs:
- output: bfloat16 [2048, 5120], P('dp')
All inputs are finite; a program needn't handle non-finite values.
Results may differ from the reference program's by a relative error of at most 0.016.
Values are sent between devices in bfloat16 or wider.
A program may use at most 2 GiB of HBM per device.

```python
import jax
import jax.numpy as jnp

ROWS = 2048
D = 5120
FF = 16384


def setup_inputs(seed: int = 0, part: int = 0) -> dict:
    kx, kg, ku, kd = jax.random.split(jax.random.key(seed), 4)
    drawn = {
        "x": jax.random.normal(jax.random.fold_in(kx, part), (ROWS, D), jnp.float32),
        "w_gate": jax.random.normal(kg, (D, FF), jnp.float32) * D**-0.5,
        "w_up": jax.random.normal(ku, (D, FF), jnp.float32) * D**-0.5,
        "w_down": jax.random.normal(kd, (FF, D), jnp.float32) * FF**-0.5,
    }
    return {k: v.astype(jnp.bfloat16) for k, v in drawn.items()}


def reference(x, w_gate, w_up, w_down):
    gate = jnp.dot(x, w_gate, preferred_element_type=jnp.float32)
    up = jnp.dot(x, w_up, preferred_element_type=jnp.float32)
    hidden = (jax.nn.silu(gate) * up).astype(jnp.bfloat16)
    return jnp.dot(hidden, w_down, preferred_element_type=jnp.float32).astype(jnp.bfloat16)
```

```python
import functools

import jax
import jax.numpy as jnp
from jax import lax
from jax.experimental import pallas as pl
from jax.experimental.pallas import tpu as pltpu
from jax.sharding import PartitionSpec as P

MESH = pl.DeviceIdType.MESH
R = 256
GT = 512
F32, BF16 = jnp.float32, jnp.bfloat16


def _dot(a, b):
    return jnp.dot(a, b, preferred_element_type=F32)


def kernel(
    x_ref, wg_ref, wu_ref, wd_ref, t_ref,
    xb, wg, wd, ring, hb, s0s, s0r, s1s, s1r, s2s, s2r, keep1, keep2, fin,
    x_sem, wg_sem, wd_sem, ring_sem,
    s0_ss, s0_rs, s1_ss, s1_rs, s2_ss, s2_rs,
    ag_ss, ag_rs, loc_sem,
    credit0, credit1, credit2,
):
    rows, d = x_ref.shape
    hid = wg_ref.shape[1]
    nc = rows // R
    nt = hid // GT
    kh = d // 2
    blk = d // 8
    nring = 3

    me = lax.axis_index("tp")
    c = lax.rem(me, 2)
    cy = lax.rem(me // 2, 2)
    cx = me // 4
    k1 = cx + c * (cy - cx)
    k2 = cy + c * (cx - cy)
    partner = me + 1 - 2 * c
    n1 = me + (1 - 2 * k1) * (4 - 2 * c)
    n2 = me + (1 - 2 * k2) * (2 + 2 * c)

    mine = 4 * c + 2 * k1 + k2
    mine_n2 = 4 * c + 2 * k1 + (1 - k2)
    far_a = 4 * c + 2 * (1 - k1) + k2
    far_b = 4 * c + 2 * (1 - k1) + (1 - k2)
    pc = 4 * (1 - c)
    p_mine = pc + 2 * k2 + k1
    p_mine_n2 = pc + 2 * k2 + (1 - k1)
    p_far = pc + 2 * (1 - k2)

    def tile(j, b, n=1):
        return t_ref.at[pl.ds(pl.multiple_of(j * R, R), R), pl.ds(pl.multiple_of(b * blk, 128), n * blk)]

    def remote(src, dst, ss, rs, to):
        return pltpu.make_async_remote_copy(
            src_ref=src, dst_ref=dst, send_sem=ss, recv_sem=rs, device_id={"tp": to}, device_id_type=MESH
        )

    def load_x(i):
        return pltpu.make_async_copy(x_ref.at[pl.ds(pl.multiple_of(i * R, R), R)], xb, x_sem)

    def load_g(t):
        return pltpu.make_async_copy(wg_ref.at[:, pl.ds(pl.multiple_of(t * GT, 128), GT)], wg.at[t], wg_sem.at[t])

    order = (
        2 * (1 - c) + (1 - k2),
        2 * c + (1 - k1),
        2 * (1 - c) + k2,
        2 * c + k1,
    )

    def load_d(o):
        col = pl.multiple_of(order[o] * (2 * blk), 128)
        return pltpu.make_async_copy(wd_ref.at[:, pl.ds(col, 2 * blk)], wd.at[o], wd_sem.at[o])

    def load_u(g):
        s = lax.rem(g, 2 * nt)
        t, half = s // 2, lax.rem(s, 2)
        slot = lax.rem(g, nring)
        src = wu_ref.at[pl.ds(pl.multiple_of(half * kh, kh), kh), pl.ds(pl.multiple_of(t * GT, 128), GT)]
        return pltpu.make_async_copy(src, ring.at[slot], ring_sem.at[slot])

    def s0(b):
        return remote(s0s.at[b], s0r.at[b], s0_ss.at[b], s0_rs.at[b], partner)

    def s1(j):
        p = lax.rem(j, 2)
        return remote(s1s.at[p], s1r.at[p], s1_ss.at[p], s1_rs.at[p], n1)

    def s2(j):
        p = lax.rem(j, 2)
        return remote(s2s.at[p], s2r.at[p], s2_ss.at[p], s2_rs.at[p], n2)

    def ag(kind, j, src, dst, to):
        return remote(src, dst, ag_ss.at[kind, j], ag_rs.at[kind, j], to)

    def fins(j):
        f = fin.at[lax.rem(j, 2)]
        dst = tile(j, mine)
        return (
            ag(0, j, f, dst, n2),
            ag(1, j, f, dst, n1),
            ag(2, j, f, dst, partner),
            pltpu.make_async_copy(f, dst, loc_sem.at[lax.rem(j, 2)]),
        )

    def wait_fins(j):
        a1, a2, a0, loc = fins(j)
        a1.wait_send()
        a2.wait_send()
        a0.wait_send()
        loc.wait()

    def passed(j):
        v = tile(j, mine_n2)
        return ag(3, j, v, v, n1), ag(4, j, v, v, partner)

    def crossed(j):
        v = tile(j, 4 * c + 2 * (1 - k1), 2)
        return ag(5, j, v, v, partner)

    def event1(j):
        s1(j).wait_recv()
        p = lax.rem(j, 2)

        @pl.when(j >= 2)
        def _():
            s2(j).wait_send()
            pl.semaphore_wait(credit2, 1)

        s2s[p] = (keep1[1 - k2] + s1r[p, 1 - k2].astype(F32)).astype(BF16)
        s2(j).start()
        keep2[...] = keep1[k2] + s1r[p, k2].astype(F32)

        @pl.when(j < nc - 2)
        def _():
            pl.semaphore_signal(credit1, inc=1, device_id={"tp": n1}, device_id_type=MESH)

    def event2(j):
        s2(j).wait_recv()
        p = lax.rem(j, 2)

        @pl.when(j >= 2)
        def _():
            wait_fins(j - 2)

        fin[p] = (keep2[...] + s2r[p].astype(F32)).astype(BF16)
        for cp in fins(j):
            cp.start()

        @pl.when(j < nc - 2)
        def _():
            pl.semaphore_signal(credit2, inc=1, device_id={"tp": n2}, device_id_type=MESH)

    def event3(j):
        v = tile(j, mine_n2)
        ag(0, j, v, v, n2).wait_recv()
        for cp in passed(j):
            cp.start()

    def event4(j):
        v = tile(j, far_a)
        ag(1, j, v, v, n1).wait_recv()
        v = tile(j, far_b)
        ag(3, j, v, v, n1).wait_recv()
        crossed(j).start()

    def finish(j):
        v = tile(j, p_mine)
        ag(2, j, v, v, partner).wait_recv()
        v = tile(j, p_mine_n2)
        ag(4, j, v, v, partner).wait_recv()
        v = tile(j, p_far, 2)
        ag(5, j, v, v, partner).wait_recv()
        for cp in passed(j):
            cp.wait_send()
        crossed(j).wait_send()

    load_x(0).start()
    load_g(0).start()
    load_u(0).start()
    load_u(1).start()
    load_g(1).start()
    load_u(2).start()

    barrier = pltpu.get_barrier_semaphore()
    for to in (partner, n1, n2):
        pl.semaphore_signal(barrier, inc=1, device_id={"tp": to}, device_id_type=MESH)
    pl.semaphore_wait(barrier, 3)

    def chunk(i, carry):
        load_x(i).wait()

        def gate_up(t, carry):
            g0 = 2 * nt * i + 2 * t

            @pl.when(i == 0)
            def _():
                load_g(t).wait()

                @pl.when(t < nt - 2)
                def _():
                    load_g(t + 2).start()

            gate = _dot(xb[...], wg[t])
            load_u(g0).wait()
            load_u(g0 + 1).wait()
            up = _dot(xb[:, :kh], ring[lax.rem(g0, nring)])
            up += _dot(xb[:, kh:], ring[lax.rem(g0 + 1, nring)])
            hb[:, pl.ds(pl.multiple_of(t * GT, 128), GT)] = (jax.nn.silu(gate) * up).astype(BF16)

            @pl.when(g0 + 3 < 2 * nt * nc)
            def _():
                load_u(g0 + 3).start()

            @pl.when(g0 + 4 < 2 * nt * nc)
            def _():
                load_u(g0 + 4).start()

            @pl.when((i == 0) & (t >= nt - 2))
            def _():
                for o in range(2):
                    @pl.when(t == nt - 2 + o)
                    def _():
                        load_d(o).start()

            @pl.when((i >= 1) & (t == 1))
            def _():
                @pl.when(i >= 2)
                def _():
                    event4(i - 2)

                event1(i - 1)

            @pl.when((i >= 1) & (t == nt - 1))
            def _():
                event2(i - 1)

            return carry

        lax.fori_loop(0, nt, gate_up, 0)

        @pl.when(i < nc - 1)
        def _():
            load_x(i + 1).start()

        for o in range(4):
            @pl.when(i == 0)
            def _():
                load_d(o).wait()
                if o < 2:
                    load_d(o + 2).start()

            b = o // 2
            if o % 2 == 0:
                @pl.when(i >= 1)
                def _():
                    s0(b).wait_send()
                    pl.semaphore_wait(credit0.at[b], 1)

                v = _dot(hb[...], wd[o]).astype(BF16)
                s0s[b, 0] = v[:, :blk]
                s0s[b, 1] = v[:, blk:]
                s0(b).start()
            else:
                v = _dot(hb[...], wd[o])
                s0(b).wait_recv()
                lo = v[:, :blk] + s0r[b, 0].astype(F32)
                hi = v[:, blk:] + s0r[b, 1].astype(F32)
                if o == 1:
                    @pl.when(i >= 2)
                    def _():
                        s1(i).wait_send()
                        pl.semaphore_wait(credit1, 1)

                    p = lax.rem(i, 2)
                    s1s[p, 0] = lo.astype(BF16)
                    s1s[p, 1] = hi.astype(BF16)
                    s1(i).start()
                else:
                    keep1[0] = lo
                    keep1[1] = hi

                @pl.when(i < nc - 1)
                def _():
                    pl.semaphore_signal(credit0.at[b], inc=1, device_id={"tp": partner}, device_id_type=MESH)

        @pl.when(i >= 1)
        def _():
            event3(i - 1)

        return carry

    lax.fori_loop(0, nc, chunk, 0)

    event1(nc - 1)
    event4(nc - 2)
    event2(nc - 1)
    event3(nc - 1)
    event4(nc - 1)
    for b in range(2):
        s0(b).wait_send()
    for j in (nc - 2, nc - 1):
        s1(j).wait_send()
        s2(j).wait_send()
        wait_fins(j)

    def last(j, carry):
        finish(j)
        return carry

    lax.fori_loop(0, nc, last, 0)


def block(x, wg, wu, wd):
    rows, d = x.shape
    hid = wg.shape[1]
    nc, blk = rows // R, d // 8
    hbm = pl.BlockSpec(memory_space=pl.ANY)
    dma, reg = pltpu.SemaphoreType.DMA, pltpu.SemaphoreType.REGULAR
    return pl.pallas_call(
        kernel,
        out_shape=jax.ShapeDtypeStruct((rows, d), BF16),
        in_specs=[hbm] * 4,
        out_specs=hbm,
        scratch_shapes=[
            pltpu.VMEM((R, d), BF16),
            pltpu.VMEM((hid // GT, d, GT), BF16),
            pltpu.VMEM((4, hid, 2 * blk), BF16),
            pltpu.VMEM((3, d // 2, GT), BF16),
            pltpu.VMEM((R, hid), BF16),
            pltpu.VMEM((2, 2, R, blk), BF16),
            pltpu.VMEM((2, 2, R, blk), BF16),
            pltpu.VMEM((2, 2, R, blk), BF16),
            pltpu.VMEM((2, 2, R, blk), BF16),
            pltpu.VMEM((2, R, blk), BF16),
            pltpu.VMEM((2, R, blk), BF16),
            pltpu.VMEM((2, R, blk), F32),
            pltpu.VMEM((R, blk), F32),
            pltpu.VMEM((2, R, blk), BF16),
            dma, dma((hid // GT,)), dma((4,)), dma((3,)),
            dma((2,)), dma((2,)), dma((2,)), dma((2,)), dma((2,)), dma((2,)),
            dma((6, nc)), dma((6, nc)), dma((2,)),
            reg((2,)), reg, reg,
        ],
        compiler_params=pltpu.CompilerParams(
            collective_id=0, has_side_effects=True, vmem_limit_bytes=67_043_328
        ),
        cost_estimate=pl.CostEstimate(
            flops=6 * rows * d * hid, bytes_accessed=2 * (12 * d * hid), transcendentals=rows * hid
        ),
        name="mlp_all_reduce",
    )(x, wg, wu, wd)


def solution(mesh):
    return jax.shard_map(
        block,
        mesh=mesh,
        in_specs=(P("dp", None), P(None, "tp"), P(None, "tp"), P("tp", None)),
        out_specs=P("dp", None),
        check_vma=False,
    )
```

```python
import functools

import jax
import jax.numpy as jnp
from jax import lax
from jax.experimental import pallas as pl
from jax.experimental.pallas import tpu as pltpu
from jax.sharding import PartitionSpec as P

MESH = pl.DeviceIdType.MESH
R = 256
GT = 512
F32, BF16 = jnp.float32, jnp.bfloat16

EVENTS = ((3, 1, 2), (1, 2, 1), (4, 4, 3), (2, 5, 1))


def _dot(a, b):
    return jnp.dot(a, b, preferred_element_type=F32)


def kernel(
    x_ref, wg_ref, wu_ref, wd_ref, y_ref, t_ref,
    xb, wg, ring, hb, s0s, s0r, s1s, s1r, s2s, s2r, keep1, keep2, fin,
    x_sem, wg_sem, wd_sem, ring_sem,
    s0_ss, s0_rs, s1_ss, s1_rs, s2_ss, s2_rs,
    ag_ss, ag_rs, loc_sem, fetch_sem,
    credit0, credit1, credit2, free,
):
    rows, d = x_ref.shape
    hid = wg_ref.shape[1]
    nc = rows // R
    nt = hid // GT
    kh = d // 2
    blk = d // 8
    nring = 3

    me = lax.axis_index("tp")
    c = lax.rem(me, 2)
    cy = lax.rem(me // 2, 2)
    cx = me // 4
    k1 = cx + c * (cy - cx)
    k2 = cy + c * (cx - cy)
    partner = me + 1 - 2 * c
    n1 = me + (1 - 2 * k1) * (4 - 2 * c)
    n2 = me + (1 - 2 * k2) * (2 + 2 * c)

    mine = 4 * c + 2 * k1 + k2
    mine_n2 = 4 * c + 2 * k1 + (1 - k2)
    far_a = 4 * c + 2 * (1 - k1) + k2
    far_b = 4 * c + 2 * (1 - k1) + (1 - k2)
    pc = 4 * (1 - c)
    p_mine = pc + 2 * k2 + k1
    p_mine_n2 = pc + 2 * k2 + (1 - k1)
    p_far = pc + 2 * (1 - k2)

    def tile(j, b, n=1):
        ref = y_ref if isinstance(j, int) and j == nc - 1 else t_ref
        return ref.at[pl.ds(pl.multiple_of(j * R, R), R), pl.ds(pl.multiple_of(b * blk, 128), n * blk)]

    def remote(src, dst, ss, rs, to):
        return pltpu.make_async_remote_copy(
            src_ref=src, dst_ref=dst, send_sem=ss, recv_sem=rs, device_id={"tp": to}, device_id_type=MESH
        )

    def load_x(i):
        return pltpu.make_async_copy(x_ref.at[pl.ds(pl.multiple_of(i * R, R), R)], xb, x_sem)

    def load_g(t):
        return pltpu.make_async_copy(wg_ref.at[:, pl.ds(pl.multiple_of(t * GT, 128), GT)], wg.at[t], wg_sem.at[t])

    order = (
        2 * (1 - c) + (1 - k2),
        2 * c + (1 - k1),
        2 * (1 - c) + k2,
        2 * c + k1,
    )

    def load_d(o):
        col = pl.multiple_of(order[o] * (2 * blk), 128)
        return pltpu.make_async_copy(wd_ref.at[:, pl.ds(col, 2 * blk)], y_ref.at[:, pl.ds(o * 2 * blk, 2 * blk)], wd_sem.at[o])

    def load_u(g):
        s = lax.rem(g, 2 * nt)
        t, half = s // 2, lax.rem(s, 2)
        slot = lax.rem(g, nring)
        src = wu_ref.at[pl.ds(pl.multiple_of(half * kh, kh), kh), pl.ds(pl.multiple_of(t * GT, 128), GT)]
        return pltpu.make_async_copy(src, ring.at[slot], ring_sem.at[slot])

    def s0(b):
        return remote(s0s.at[b], s0r.at[b], s0_ss.at[b], s0_rs.at[b], partner)

    def s1(j):
        p = lax.rem(j, 2)
        return remote(s1s.at[p], s1r.at[p], s1_ss.at[p], s1_rs.at[p], n1)

    def s2(j):
        p = lax.rem(j, 2)
        return remote(s2s.at[p], s2r.at[p], s2_ss.at[p], s2_rs.at[p], n2)

    def ag(kind, j, src, dst, to):
        return remote(src, dst, ag_ss.at[kind, j], ag_rs.at[kind, j], to)

    def fins(j):
        f = fin.at[lax.rem(j, 2)]
        dst = tile(j, mine)
        return (
            ag(0, j, f, dst, n2),
            ag(1, j, f, dst, n1),
            ag(2, j, f, dst, partner),
            pltpu.make_async_copy(f, dst, loc_sem.at[lax.rem(j, 2)]),
        )

    def wait_fins(j):
        a1, a2, a0, loc = fins(j)
        a1.wait_send()
        a2.wait_send()
        a0.wait_send()
        loc.wait()

    def passed(j):
        v = tile(j, mine_n2)
        return ag(3, j, v, v, n1), ag(4, j, v, v, partner)

    def crossed(j):
        v = tile(j, 4 * c + 2 * (1 - k1), 2)
        return ag(5, j, v, v, partner)

    def event1(j):
        s1(j).wait_recv()
        p = lax.rem(j, 2)

        @pl.when(j >= 2)
        def _():
            s2(j).wait_send()
            pl.semaphore_wait(credit2, 1)

        s2s[p] = (keep1[1 - k2] + s1r[p, 1 - k2].astype(F32)).astype(BF16)
        s2(j).start()
        keep2[...] = keep1[k2] + s1r[p, k2].astype(F32)

        @pl.when(j < nc - 2)
        def _():
            pl.semaphore_signal(credit1, inc=1, device_id={"tp": n1}, device_id_type=MESH)

    def event2(j):
        s2(j).wait_recv()
        p = lax.rem(j, 2)

        @pl.when(j >= 2)
        def _():
            wait_fins(j - 2)

        fin[p] = (keep2[...] + s2r[p].astype(F32)).astype(BF16)
        if isinstance(j, int) and j == nc - 1:
            for b in range(3):
                pl.semaphore_wait(free.at[b], 1)
        for cp in fins(j):
            cp.start()

        @pl.when(j < nc - 2)
        def _():
            pl.semaphore_signal(credit2, inc=1, device_id={"tp": n2}, device_id_type=MESH)

    def event3(j):
        v = tile(j, mine_n2)
        ag(0, j, v, v, n2).wait_recv()
        for cp in passed(j):
            cp.start()

    def event4(j):
        v = tile(j, far_a)
        ag(1, j, v, v, n1).wait_recv()
        v = tile(j, far_b)
        ag(3, j, v, v, n1).wait_recv()
        crossed(j).start()

    def event5(j):
        if isinstance(j, int) and j >= nc - 2:
            wait_fins(j)
        v = tile(j, p_mine)
        ag(2, j, v, v, partner).wait_recv()
        v = tile(j, p_mine_n2)
        ag(4, j, v, v, partner).wait_recv()
        v = tile(j, p_far, 2)
        ag(5, j, v, v, partner).wait_recv()
        for cp in passed(j):
            cp.wait_send()
        crossed(j).wait_send()
        if not (isinstance(j, int) and j == nc - 1):
            fetch(j).start()

    def fetch(j):
        rows_j = pl.ds(pl.multiple_of(j * R, R), R)
        return pltpu.make_async_copy(t_ref.at[rows_j], y_ref.at[rows_j], fetch_sem.at[j])

    def run(event, j):
        (event1, event2, event3, event4, event5)[event - 1](j)

    load_x(0).start()
    load_g(0).start()
    load_u(0).start()
    load_u(1).start()
    load_g(1).start()
    load_u(2).start()

    barrier = pltpu.get_barrier_semaphore()
    for to in (partner, n1, n2):
        pl.semaphore_signal(barrier, inc=1, device_id={"tp": to}, device_id_type=MESH)
    pl.semaphore_wait(barrier, 3)

    def chunk(i, carry):
        load_x(i).wait()

        def gate_up(t, carry):
            g0 = 2 * nt * i + 2 * t

            @pl.when(i == 0)
            def _():
                load_g(t).wait()

                @pl.when(t < nt - 2)
                def _():
                    load_g(t + 2).start()

            gate = _dot(xb[...], wg[t])
            load_u(g0).wait()
            load_u(g0 + 1).wait()
            up = _dot(xb[:, :kh], ring[lax.rem(g0, nring)])
            up += _dot(xb[:, kh:], ring[lax.rem(g0 + 1, nring)])
            hb[:, pl.ds(pl.multiple_of(t * GT, 128), GT)] = (jax.nn.silu(gate) * up).astype(BF16)

            @pl.when(g0 + 3 < 2 * nt * nc)
            def _():
                load_u(g0 + 3).start()

            @pl.when(g0 + 4 < 2 * nt * nc)
            def _():
                load_u(g0 + 4).start()

            @pl.when((i == 0) & (t >= nt - 2))
            def _():
                for o in range(2):
                    @pl.when(t == nt - 2 + o)
                    def _():
                        load_d(o).start()

            for event, slot, lag in EVENTS:
                if slot < nt:
                    @pl.when((i >= lag) & (t == slot))
                    def _():
                        run(event, i - lag)

            return carry

        lax.fori_loop(0, nt, gate_up, 0)

        @pl.when(i < nc - 1)
        def _():
            load_x(i + 1).start()

        for o in range(4):
            @pl.when(i == 0)
            def _():
                load_d(o).wait()
                if o < 2:
                    load_d(o + 2).start()

            b = o // 2
            if o % 2 == 0:
                @pl.when(i >= 1)
                def _():
                    s0(b).wait_send()
                    pl.semaphore_wait(credit0.at[b], 1)

                v = _dot(hb[...], y_ref[:, o * 2 * blk : (o + 1) * 2 * blk]).astype(BF16)
                s0s[b, 0] = v[:, :blk]
                s0s[b, 1] = v[:, blk:]
                s0(b).start()
            else:
                v = _dot(hb[...], y_ref[:, o * 2 * blk : (o + 1) * 2 * blk])
                s0(b).wait_recv()
                lo = v[:, :blk] + s0r[b, 0].astype(F32)
                hi = v[:, blk:] + s0r[b, 1].astype(F32)
                if o == 1:
                    @pl.when(i >= 2)
                    def _():
                        s1(i).wait_send()
                        pl.semaphore_wait(credit1, 1)

                    p = lax.rem(i, 2)
                    s1s[p, 0] = lo.astype(BF16)
                    s1s[p, 1] = hi.astype(BF16)
                    s1(i).start()
                else:
                    keep1[0] = lo
                    keep1[1] = hi

                @pl.when(i < nc - 1)
                def _():
                    pl.semaphore_signal(credit0.at[b], inc=1, device_id={"tp": partner}, device_id_type=MESH)

            for event, slot, lag in EVENTS:
                if slot == nt + o:
                    @pl.when(i >= lag)
                    def _():
                        run(event, i - lag)

        return carry

    lax.fori_loop(0, nc, chunk, 0)

    for b, to in enumerate((partner, n1, n2)):
        pl.semaphore_signal(free.at[b], inc=1, device_id={"tp": to}, device_id_type=MESH)

    def early(j, carry):
        event5(j)
        return carry

    lax.fori_loop(0, nc - 3, early, 0)
    rest = [(j + 4, 0, 5, j) for j in range(nc - 3, nc)]
    for event, slot, lag in EVENTS:
        for j in range(nc - lag, nc):
            rest.append((j + lag, slot, event, j))
    for _, _, event, j in sorted(rest):
        run(event, j)

    for b in range(2):
        s0(b).wait_send()
    for j in (nc - 2, nc - 1):
        s1(j).wait_send()
        s2(j).wait_send()

    def fetched(j, carry):
        fetch(j).wait()
        return carry

    lax.fori_loop(0, nc - 1, fetched, 0)


def block(x, wg, wu, wd):
    rows, d = x.shape
    hid = wg.shape[1]
    nc, blk = rows // R, d // 8
    hbm = pl.BlockSpec(memory_space=pl.ANY)
    dma, reg = pltpu.SemaphoreType.DMA, pltpu.SemaphoreType.REGULAR
    return pl.pallas_call(
        kernel,
        out_shape=(pltpu.VMEM((rows, d), BF16), jax.ShapeDtypeStruct((rows, d), BF16)),
        in_specs=[hbm] * 4,
        out_specs=(pl.BlockSpec(memory_space=pltpu.VMEM), hbm),
        scratch_shapes=[
            pltpu.VMEM((R, d), BF16),
            pltpu.VMEM((hid // GT, d, GT), BF16),
            pltpu.VMEM((3, d // 2, GT), BF16),
            pltpu.VMEM((R, hid), BF16),
            pltpu.VMEM((2, 2, R, blk), BF16),
            pltpu.VMEM((2, 2, R, blk), BF16),
            pltpu.VMEM((2, 2, R, blk), BF16),
            pltpu.VMEM((2, 2, R, blk), BF16),
            pltpu.VMEM((2, R, blk), BF16),
            pltpu.VMEM((2, R, blk), BF16),
            pltpu.VMEM((2, R, blk), F32),
            pltpu.VMEM((R, blk), F32),
            pltpu.VMEM((2, R, blk), BF16),
            dma, dma((hid // GT,)), dma((4,)), dma((3,)),
            dma((2,)), dma((2,)), dma((2,)), dma((2,)), dma((2,)), dma((2,)),
            dma((6, nc)), dma((6, nc)), dma((2,)), dma((nc,)),
            reg((2,)), reg, reg, reg((3,)),
        ],
        compiler_params=pltpu.CompilerParams(
            collective_id=0, has_side_effects=True, vmem_limit_bytes=67_043_328 - 2 * rows * d
        ),
        cost_estimate=pl.CostEstimate(
            flops=6 * rows * d * hid, bytes_accessed=2 * (12 * d * hid), transcendentals=rows * hid
        ),
        name="mlp_all_reduce",
    )(x, wg, wu, wd)[0]


def solution(mesh):
    return jax.shard_map(
        block,
        mesh=mesh,
        in_specs=(P("dp", None), P(None, "tp"), P(None, "tp"), P("tp", None)),
        out_specs=P("dp", None),
        check_vma=False,
    )
```

```python
import functools

import jax
import jax.numpy as jnp
from jax import lax
from jax.experimental import pallas as pl
from jax.experimental.pallas import tpu as pltpu
from jax.sharding import PartitionSpec as P

MESH = pl.DeviceIdType.MESH
R = 256
RB = 64
NT = 256
GT = 512
F32, BF16 = jnp.float32, jnp.bfloat16

EVENTS = ((1, 3, 1), (2, 0, 2), (3, 6, 2), (4, 5, 3))
FIRST = ((1, 2, 1), (2, 4, 1), (3, 1, 2), (4, 4, 3))
DRAIN = ((2, 1), (1, 0), (3, 1), (4, 2), (2, 0), (5, 2), (3, 0), (4, 1), (5, 1), (4, 0), (5, 0))


def _dot(a, b):
    return jnp.dot(a, b, preferred_element_type=F32)


def kernel(
    x_ref, wg_ref, wu_ref, wd_ref, y_ref, t_ref,
    xb, wg, ring, hb, s0s, s0r, s1s, s1r, s2s, s2r, keep1, keep2, fin,
    x_sem, wg_sem, wd_sem, ring_sem,
    s0_ss, s0_rs, s1_ss, s1_rs, s2_ss, s2_rs,
    ag_ss, ag_rs, loc_sem, fetch_sem,
    credit0, credit1, credit2, free,
):
    rows, d = x_ref.shape
    hid = wg_ref.shape[1]
    nc = rows // R
    nt = hid // GT
    parts = [slice(k, k + R // 2) for k in (0, R // 2)]
    blk = d // 8

    me = lax.axis_index("tp")
    c = lax.rem(me, 2)
    cy = lax.rem(me // 2, 2)
    cx = me // 4
    k1 = cx + c * (cy - cx)
    k2 = cy + c * (cx - cy)
    partner = me + 1 - 2 * c
    n1 = me + (1 - 2 * k1) * (4 - 2 * c)
    n2 = me + (1 - 2 * k2) * (2 + 2 * c)

    mine = 4 * c + 2 * k1 + k2
    mine_n2 = 4 * c + 2 * k1 + (1 - k2)
    far_a = 4 * c + 2 * (1 - k1) + k2
    far_b = 4 * c + 2 * (1 - k1) + (1 - k2)
    pc = 4 * (1 - c)
    p_mine = pc + 2 * k2 + k1
    p_mine_n2 = pc + 2 * k2 + (1 - k1)
    p_far = pc + 2 * (1 - k2)

    def tile(j, b, n=1):
        ref = y_ref if isinstance(j, int) and j == nc - 1 else t_ref
        return ref.at[pl.ds(pl.multiple_of(j * R, R), R), pl.ds(pl.multiple_of(b * blk, 128), n * blk)]

    def remote(src, dst, ss, rs, to):
        return pltpu.make_async_remote_copy(
            src_ref=src, dst_ref=dst, send_sem=ss, recv_sem=rs, device_id={"tp": to}, device_id_type=MESH
        )

    def load_x(i):
        return pltpu.make_async_copy(x_ref.at[pl.ds(pl.multiple_of(i * R, R), R)], xb, x_sem)

    def load_g(t):
        return pltpu.make_async_copy(wg_ref.at[:, pl.ds(pl.multiple_of(t * GT, 128), GT)], wg.at[t], wg_sem.at[t])

    order = (
        2 * (1 - c) + (1 - k2),
        2 * (1 - c) + k2,
        2 * c + (1 - k1),
        2 * c + k1,
    )

    def load_d(o):
        col = pl.multiple_of(order[o] * (2 * blk), 128)
        return pltpu.make_async_copy(wd_ref.at[:, pl.ds(col, 2 * blk)], y_ref.at[:, pl.ds(o * 2 * blk, 2 * blk)], wd_sem.at[o])

    def load_u(g):
        t, slot = lax.rem(g, nt), lax.rem(g, 2)
        src = wu_ref.at[:, pl.ds(pl.multiple_of(t * GT, 128), GT)]
        return pltpu.make_async_copy(src, ring.at[slot], ring_sem.at[slot])

    def s0(b):
        return remote(s0s.at[b], s0r.at[b], s0_ss.at[b], s0_rs.at[b], partner)

    def s1():
        return remote(s1s, s1r, s1_ss, s1_rs, n1)

    def s2():
        return remote(s2s, s2r, s2_ss, s2_rs, n2)

    def ag(kind, j, src, dst, to):
        return remote(src, dst, ag_ss.at[kind, j], ag_rs.at[kind, j], to)

    def fins(j):
        f = fin.at[lax.rem(j, 2)]
        dst = tile(j, mine)
        return (
            ag(0, j, f, dst, n2),
            ag(1, j, f, dst, n1),
            ag(2, j, f, dst, partner),
            pltpu.make_async_copy(f, dst, loc_sem.at[lax.rem(j, 2)]),
        )

    def wait_fins(j):
        a1, a2, a0, loc = fins(j)
        a1.wait_send()
        a2.wait_send()
        a0.wait_send()
        loc.wait()

    def passed(j):
        v = tile(j, mine_n2)
        return ag(3, j, v, v, n1), ag(4, j, v, v, partner)

    def crossed(j):
        v = tile(j, 4 * c + 2 * (1 - k1), 2)
        return ag(5, j, v, v, partner)

    def by_rows(f):
        def body(q, carry):
            f(pl.ds(pl.multiple_of(q * RB, RB), RB))
            return carry

        lax.fori_loop(0, R // RB, body, 0)

    def event1(j):
        s1().wait_recv()

        @pl.when(j >= 1)
        def _():
            s2().wait_send()
            pl.semaphore_wait(credit2, 1)

        def send_half(q):
            s2s[q] = (keep1[1 - k2, q] + s1r[1 - k2, q].astype(F32)).astype(BF16)

        def keep_half(q):
            keep2[q] = keep1[k2, q] + s1r[k2, q].astype(F32)

        by_rows(send_half)
        s2().start()
        by_rows(keep_half)

        @pl.when(j < nc - 1)
        def _():
            pl.semaphore_signal(credit1, inc=1, device_id={"tp": n1}, device_id_type=MESH)

    def event2(j):
        s2().wait_recv()
        p = lax.rem(j, 2)

        @pl.when(j >= 2)
        def _():
            wait_fins(j - 2)

        def total(q):
            fin[p, q] = (keep2[q] + s2r[q].astype(F32)).astype(BF16)

        by_rows(total)
        if isinstance(j, int) and j == nc - 1:
            for b in range(3):
                pl.semaphore_wait(free.at[b], 1)
        for cp in fins(j):
            cp.start()

        @pl.when(j < nc - 1)
        def _():
            pl.semaphore_signal(credit2, inc=1, device_id={"tp": n2}, device_id_type=MESH)

    def event3(j):
        v = tile(j, mine_n2)
        ag(0, j, v, v, n2).wait_recv()
        for cp in passed(j):
            cp.start()

    def event4(j):
        v = tile(j, far_a)
        ag(1, j, v, v, n1).wait_recv()
        v = tile(j, far_b)
        ag(3, j, v, v, n1).wait_recv()
        crossed(j).start()

    def event5(j):
        if isinstance(j, int) and j >= nc - 2:
            wait_fins(j)
        v = tile(j, p_mine)
        ag(2, j, v, v, partner).wait_recv()
        v = tile(j, p_mine_n2)
        ag(4, j, v, v, partner).wait_recv()
        v = tile(j, p_far, 2)
        ag(5, j, v, v, partner).wait_recv()
        for cp in passed(j):
            cp.wait_send()
        crossed(j).wait_send()
        if not (isinstance(j, int) and j == nc - 1):
            fetch(j).start()

    def fetch(j):
        rows_j = pl.ds(pl.multiple_of(j * R, R), R)
        return pltpu.make_async_copy(t_ref.at[rows_j], y_ref.at[rows_j], fetch_sem.at[j])

    def run(event, j):
        (event1, event2, event3, event4, event5)[event - 1](j)

    def at_slot(slot, i, here):
        for event, s, lag in FIRST:
            if s == slot:
                @pl.when(here & (i == lag))
                def _():
                    run(event, 0)

        for event, s, lag in EVENTS:
            if s == slot:
                @pl.when(here & (i > lag))
                def _():
                    run(event, i - lag)

    load_x(0).start()
    load_g(0).start()
    load_u(0).start()

    barrier = pltpu.get_barrier_semaphore()
    for to in (partner, n1, n2):
        pl.semaphore_signal(barrier, inc=1, device_id={"tp": to}, device_id_type=MESH)
    pl.semaphore_wait(barrier, 3)

    def down(o, put):
        for q in parts:
            for lo in range(0, 2 * blk, NT):
                v = _dot(hb[q], y_ref[:, o * 2 * blk + lo : o * 2 * blk + lo + NT])
                for h in range(2):
                    first, end = max(lo, h * blk), min(lo + NT, (h + 1) * blk)
                    if first < end:
                        put(h, q, slice(first - h * blk, end - h * blk), v[:, first - lo : end - lo])

    def chunk(i, carry):
        load_x(i).wait()

        def gate_up(t, carry):
            g = nt * i + t

            @pl.when(i == 0)
            def _():
                load_g(t).wait()

                @pl.when(t < nt - 1)
                def _():
                    load_g(t + 1).start()

            load_u(g).wait()

            @pl.when(g + 1 < nt * nc)
            def _():
                load_u(g + 1).start()

            @pl.when((i == 0) & (t == nt - 1))
            def _():
                for o in range(3):
                    load_d(o).start()

            cols = pl.ds(pl.multiple_of(t * GT, 128), GT)
            slot = lax.rem(g, 2)
            for q in parts:
                gate = _dot(xb[q], wg[t])
                up = _dot(xb[q], ring[slot])
                hb[q, cols] = (jax.nn.silu(gate) * up).astype(BF16)

            for slot in range(nt):
                at_slot(slot, i, t == slot)

            return carry

        lax.fori_loop(0, nt, gate_up, 0)

        @pl.when(i < nc - 1)
        def _():
            load_x(i + 1).start()

        for o in range(4):
            @pl.when(i == 0)
            def _():
                load_d(o).wait()
                if o == 0:
                    load_d(3).start()

            b = o % 2
            if o < 2:
                @pl.when(i >= 1)
                def _():
                    s0(b).wait_send()
                    pl.semaphore_wait(credit0.at[b], 1)

                def put(h, q, cols, v):
                    s0s[b, h, q, cols] = v.astype(BF16)

                down(o, put)
                s0(b).start()
            else:
                if o == 2:
                    @pl.when(i >= 1)
                    def _():
                        s1().wait_send()
                        pl.semaphore_wait(credit1, 1)

                s0(b).wait_recv()
                def put(h, q, cols, v):
                    v += s0r[b, h, q, cols].astype(F32)
                    if o == 2:
                        s1s[h, q, cols] = v.astype(BF16)
                    else:
                        keep1[h, q, cols] = v

                down(o, put)
                if o == 2:
                    s1().start()

                @pl.when(i < nc - 1)
                def _():
                    pl.semaphore_signal(credit0.at[b], inc=1, device_id={"tp": partner}, device_id_type=MESH)

            at_slot(nt + o, i, i >= 0)

        return carry

    lax.fori_loop(0, nc, chunk, 0)

    for b, to in enumerate((partner, n1, n2)):
        pl.semaphore_signal(free.at[b], inc=1, device_id={"tp": to}, device_id_type=MESH)

    def early(j, carry):
        event5(j)
        return carry

    for k, (event, back) in enumerate(DRAIN):
        run(event, nc - 1 - back)
        if k == 0:
            lax.fori_loop(0, nc - 3, early, 0)

    for b in range(2):
        s0(b).wait_send()
    s1().wait_send()
    s2().wait_send()

    def fetched(j, carry):
        fetch(j).wait()
        return carry

    lax.fori_loop(0, nc - 1, fetched, 0)


def block(x, wg, wu, wd):
    rows, d = x.shape
    hid = wg.shape[1]
    nc, blk = rows // R, d // 8
    hbm = pl.BlockSpec(memory_space=pl.ANY)
    dma, reg = pltpu.SemaphoreType.DMA, pltpu.SemaphoreType.REGULAR
    return pl.pallas_call(
        kernel,
        out_shape=(pltpu.VMEM((rows, d), BF16), jax.ShapeDtypeStruct((rows, d), BF16)),
        in_specs=[hbm] * 4,
        out_specs=(pl.BlockSpec(memory_space=pltpu.VMEM), hbm),
        scratch_shapes=[
            pltpu.VMEM((R, d), BF16),
            pltpu.VMEM((hid // GT, d, GT), BF16),
            pltpu.VMEM((2, d, GT), BF16),
            pltpu.VMEM((R, hid), BF16),
            pltpu.VMEM((2, 2, R, blk), BF16),
            pltpu.VMEM((2, 2, R, blk), BF16),
            pltpu.VMEM((2, R, blk), BF16),
            pltpu.VMEM((2, R, blk), BF16),
            pltpu.VMEM((R, blk), BF16),
            pltpu.VMEM((R, blk), BF16),
            pltpu.VMEM((2, R, blk), F32),
            pltpu.VMEM((R, blk), F32),
            pltpu.VMEM((2, R, blk), BF16),
            dma, dma((hid // GT,)), dma((4,)), dma((2,)),
            dma((2,)), dma((2,)), dma, dma, dma, dma,
            dma((6, nc)), dma((6, nc)), dma((2,)), dma((nc,)),
            reg((2,)), reg, reg, reg((3,)),
        ],
        compiler_params=pltpu.CompilerParams(
            collective_id=0, has_side_effects=True, vmem_limit_bytes=67_043_328 - 2 * rows * d
        ),
        cost_estimate=pl.CostEstimate(
            flops=6 * rows * d * hid, bytes_accessed=2 * (12 * d * hid), transcendentals=rows * hid
        ),
        name="mlp_all_reduce",
    )(x, wg, wu, wd)[0]


def solution(mesh):
    return jax.shard_map(
        block,
        mesh=mesh,
        in_specs=(P("dp", None), P(None, "tp"), P(None, "tp"), P("tp", None)),
        out_specs=P("dp", None),
        check_vma=False,
    )
```

```python
import functools

import jax
import jax.numpy as jnp
from jax import lax
from jax.experimental import pallas as pl
from jax.experimental.pallas import tpu as pltpu
from jax.sharding import PartitionSpec as P

MESH = pl.DeviceIdType.MESH
R = 256
RB = 64
NT = 256
GT = 512
F32, BF16 = jnp.float32, jnp.bfloat16

EVENTS = ((10, 12, 18, 28), (11, 16, 22, 29))
DRAIN = ((2, 1), (1, 0), (3, 1), (4, 2), (2, 0), (5, 2), (3, 0), (4, 1), (5, 1), (4, 0), (5, 0))


def _dot(a, b):
    return jnp.dot(a, b, preferred_element_type=F32)


def kernel(
    x_ref, wg_ref, wu_ref, wd_ref, y_ref, t_ref,
    xb, wg, ring, hb, s0s, s0r, s1s, s1r, s2s, s2r, keep1, keep2, fin,
    x_sem, wg_sem, wd_sem, ring_sem,
    s0_ss, s0_rs, s1_ss, s1_rs, s2_ss, s2_rs,
    ag_ss, ag_rs, loc_sem, fetch_sem,
    credit0, credit1, credit2, free,
):
    rows, d = x_ref.shape
    hid = wg_ref.shape[1]
    nc = rows // R
    nt = hid // GT
    parts = [slice(k, k + R // 2) for k in (0, R // 2)]
    blk = d // 8

    me = lax.axis_index("tp")
    c = lax.rem(me, 2)
    cy = lax.rem(me // 2, 2)
    cx = me // 4
    k1 = cx + c * (cy - cx)
    k2 = cy + c * (cx - cy)
    partner = me + 1 - 2 * c
    n1 = me + (1 - 2 * k1) * (4 - 2 * c)
    n2 = me + (1 - 2 * k2) * (2 + 2 * c)

    mine = 4 * c + 2 * k1 + k2
    mine_n2 = 4 * c + 2 * k1 + (1 - k2)
    far_a = 4 * c + 2 * (1 - k1) + k2
    far_b = 4 * c + 2 * (1 - k1) + (1 - k2)
    pc = 4 * (1 - c)
    p_mine = pc + 2 * k2 + k1
    p_mine_n2 = pc + 2 * k2 + (1 - k1)
    p_far = pc + 2 * (1 - k2)

    def is_last(j):
        return isinstance(j, int) and j == nc - 1

    def tile(j, b, n=1):
        ref = y_ref if is_last(j) else t_ref
        return ref.at[pl.ds(pl.multiple_of(j * R, R), R), pl.ds(pl.multiple_of(b * blk, 128), n * blk)]

    def remote(src, dst, ss, rs, to):
        return pltpu.make_async_remote_copy(
            src_ref=src, dst_ref=dst, send_sem=ss, recv_sem=rs, device_id={"tp": to}, device_id_type=MESH
        )

    def load_x(i):
        return pltpu.make_async_copy(x_ref.at[pl.ds(pl.multiple_of(i * R, R), R)], xb, x_sem)

    def load_g(t):
        return pltpu.make_async_copy(wg_ref.at[:, pl.ds(pl.multiple_of(t * GT, 128), GT)], wg.at[t], wg_sem.at[t])

    order = (
        2 * (1 - c) + (1 - k2),
        2 * (1 - c) + k2,
        2 * c + (1 - k1),
        2 * c + k1,
    )

    def load_d(o):
        col = pl.multiple_of(order[o] * (2 * blk), 128)
        return pltpu.make_async_copy(wd_ref.at[:, pl.ds(col, 2 * blk)], y_ref.at[:, pl.ds(o * 2 * blk, 2 * blk)], wd_sem.at[o])

    def load_u(g):
        t, slot = lax.rem(g, nt), lax.rem(g, 2)
        src = wu_ref.at[:, pl.ds(pl.multiple_of(t * GT, 128), GT)]
        return pltpu.make_async_copy(src, ring.at[slot], ring_sem.at[slot])

    def s0(b):
        return remote(s0s.at[b], s0r.at[b], s0_ss.at[b], s0_rs.at[b], partner)

    def s1():
        return remote(s1s, s1r, s1_ss, s1_rs, n1)

    def s2():
        return remote(s2s, s2r, s2_ss, s2_rs, n2)

    def ag(kind, j, src, dst, to):
        return remote(src, dst, ag_ss.at[kind, j], ag_rs.at[kind, j], to)

    def fins(j):
        f = fin.at[lax.rem(j, 2)]
        dst = tile(j, mine)
        return (
            ag(0, j, f, dst, n2),
            ag(1, j, f, dst, n1),
            ag(2, j, f, dst, partner),
            pltpu.make_async_copy(f, dst, loc_sem.at[lax.rem(j, 2)]),
        )

    def wait_fins(j):
        a1, a2, a0, loc = fins(j)
        a1.wait_send()
        a2.wait_send()
        a0.wait_send()
        loc.wait()

    def passed(j):
        v = tile(j, mine_n2)
        return ag(3, j, v, v, n1), ag(4, j, v, v, partner)

    def crossed(j):
        if is_last(j):
            va, vb = tile(j, far_a), tile(j, far_b)
            return ag(5, j, va, va, partner), ag(6, j, vb, vb, partner)
        v = tile(j, 4 * c + 2 * (1 - k1), 2)
        return (ag(5, j, v, v, partner),)

    def by_rows(f):
        def body(q, carry):
            f(pl.ds(pl.multiple_of(q * RB, RB), RB))
            return carry

        lax.fori_loop(0, R // RB, body, 0)

    def event1(j):
        s1().wait_recv()

        @pl.when(j >= 1)
        def _():
            s2().wait_send()
            pl.semaphore_wait(credit2, 1)

        def send_half(q):
            s2s[q] = (keep1[1 - k2, q] + s1r[1 - k2, q].astype(F32)).astype(BF16)

        def keep_half(q):
            keep2[q] = keep1[k2, q] + s1r[k2, q].astype(F32)

        by_rows(send_half)
        s2().start()
        by_rows(keep_half)

        @pl.when(j < nc - 1)
        def _():
            pl.semaphore_signal(credit1, inc=1, device_id={"tp": n1}, device_id_type=MESH)

    def event2(j):
        s2().wait_recv()
        p = lax.rem(j, 2)

        @pl.when(j >= 2)
        def _():
            wait_fins(j - 2)

        def total(q):
            fin[p, q] = (keep2[q] + s2r[q].astype(F32)).astype(BF16)

        by_rows(total)
        if is_last(j):
            for b in range(3):
                pl.semaphore_wait(free.at[b], 1)
        a1, a2, a0, loc = fins(j)
        a1.start()
        a0.start()
        loc.start()
        a2.start()

        @pl.when(j < nc - 1)
        def _():
            pl.semaphore_signal(credit2, inc=1, device_id={"tp": n2}, device_id_type=MESH)

    def event3(j):
        v = tile(j, mine_n2)
        ag(0, j, v, v, n2).wait_recv()
        for cp in passed(j):
            cp.start()

    def event4(j):
        sends = crossed(j)
        v = tile(j, far_a)
        ag(1, j, v, v, n1).wait_recv()
        if is_last(j):
            sends[0].start()
        v = tile(j, far_b)
        ag(3, j, v, v, n1).wait_recv()
        sends[-1].start()

    def event5(j):
        if isinstance(j, int) and j >= nc - 2:
            wait_fins(j)
        v = tile(j, p_mine)
        ag(2, j, v, v, partner).wait_recv()
        v = tile(j, p_mine_n2)
        ag(4, j, v, v, partner).wait_recv()
        if is_last(j):
            v = tile(j, p_far + k1)
            ag(5, j, v, v, partner).wait_recv()
            v = tile(j, p_far + (1 - k1))
            ag(6, j, v, v, partner).wait_recv()
        else:
            v = tile(j, p_far, 2)
            ag(5, j, v, v, partner).wait_recv()
        for cp in passed(j):
            cp.wait_send()
        for cp in crossed(j):
            cp.wait_send()
        if not is_last(j):
            fetch(j).start()

    def fetch(j):
        rows_j = pl.ds(pl.multiple_of(j * R, R), R)
        return pltpu.make_async_copy(t_ref.at[rows_j], y_ref.at[rows_j], fetch_sem.at[j])

    def run(event, j):
        (event1, event2, event3, event4, event5)[event - 1](j)

    def at_slot(slot, i, here):
        for first, row in enumerate(EVENTS):
            for event, place in enumerate(row, 1):
                if place % 8 == slot:
                    j = i - place // 8
                    mine_now = j >= first if first == len(EVENTS) - 1 else j == first

                    @pl.when(here & mine_now)
                    def _():
                        run(event, j)

    load_x(0).start()
    load_g(0).start()
    load_u(0).start()

    barrier = pltpu.get_barrier_semaphore()
    for to in (partner, n1, n2):
        pl.semaphore_signal(barrier, inc=1, device_id={"tp": to}, device_id_type=MESH)
    pl.semaphore_wait(barrier, 3)

    def down(o, put):
        for q in parts:
            for lo in range(0, 2 * blk, NT):
                v = _dot(hb[q], y_ref[:, o * 2 * blk + lo : o * 2 * blk + lo + NT])
                for h in range(2):
                    first, end = max(lo, h * blk), min(lo + NT, (h + 1) * blk)
                    if first < end:
                        put(h, q, slice(first - h * blk, end - h * blk), v[:, first - lo : end - lo])

    def chunk(i, carry):
        load_x(i).wait()

        def gate_up(t, carry):
            g = nt * i + t

            @pl.when(i == 0)
            def _():
                load_g(t).wait()

                @pl.when(t < nt - 1)
                def _():
                    load_g(t + 1).start()

            load_u(g).wait()

            @pl.when(g + 1 < nt * nc)
            def _():
                load_u(g + 1).start()

            @pl.when((i == 0) & (t == nt - 1))
            def _():
                for o in range(3):
                    load_d(o).start()

            cols = pl.ds(pl.multiple_of(t * GT, 128), GT)
            slot = lax.rem(g, 2)
            for q in parts:
                gate = _dot(xb[q], wg[t])
                up = _dot(xb[q], ring[slot])
                hb[q, cols] = (jax.nn.silu(gate) * up).astype(BF16)

            for slot in range(nt):
                at_slot(slot, i, t == slot)

            return carry

        lax.fori_loop(0, nt, gate_up, 0)

        for o in range(4):
            @pl.when(i == 0)
            def _():
                load_d(o).wait()
                if o == 0:
                    load_d(3).start()

            b = o % 2
            if o == 2:
                @pl.when(i < nc - 1)
                def _():
                    load_x(i + 1).start()

            if o < 2:
                @pl.when(i >= 1)
                def _():
                    s0(b).wait_send()
                    pl.semaphore_wait(credit0.at[b], 1)

                def put(h, q, cols, v):
                    s0s[b, h, q, cols] = v.astype(BF16)

                down(o, put)
                s0(b).start()
            else:
                if o == 2:
                    @pl.when(i >= 1)
                    def _():
                        s1().wait_send()
                        pl.semaphore_wait(credit1, 1)

                s0(b).wait_recv()
                def put(h, q, cols, v):
                    v += s0r[b, h, q, cols].astype(F32)
                    if o == 2:
                        s1s[h, q, cols] = v.astype(BF16)
                    else:
                        keep1[h, q, cols] = v

                down(o, put)
                if o == 2:
                    s1().start()

                @pl.when(i < nc - 1)
                def _():
                    pl.semaphore_signal(credit0.at[b], inc=1, device_id={"tp": partner}, device_id_type=MESH)

            at_slot(nt + o, i, i >= 0)

        return carry

    lax.fori_loop(0, nc, chunk, 0)

    for b, to in enumerate((partner, n1, n2)):
        pl.semaphore_signal(free.at[b], inc=1, device_id={"tp": to}, device_id_type=MESH)

    def early(j, carry):
        event5(j)
        return carry

    lag_of = {event: place // 8 for event, place in enumerate(EVENTS[-1], 1)} | {5: nc}
    for event, back in DRAIN:
        if (event, back) == (3, 1):
            lax.fori_loop(0, nc - 3, early, 0)
        if back < lag_of[event]:
            run(event, nc - 1 - back)

    for b in range(2):
        s0(b).wait_send()
    s1().wait_send()
    s2().wait_send()

    def fetched(j, carry):
        fetch(j).wait()
        return carry

    lax.fori_loop(0, nc - 1, fetched, 0)


def block(x, wg, wu, wd):
    rows, d = x.shape
    hid = wg.shape[1]
    nc, blk = rows // R, d // 8
    hbm = pl.BlockSpec(memory_space=pl.ANY)
    dma, reg = pltpu.SemaphoreType.DMA, pltpu.SemaphoreType.REGULAR
    return pl.pallas_call(
        kernel,
        out_shape=(pltpu.VMEM((rows, d), BF16), jax.ShapeDtypeStruct((rows, d), BF16)),
        in_specs=[hbm] * 4,
        out_specs=(pl.BlockSpec(memory_space=pltpu.VMEM), hbm),
        scratch_shapes=[
            pltpu.VMEM((R, d), BF16),
            pltpu.VMEM((hid // GT, d, GT), BF16),
            pltpu.VMEM((2, d, GT), BF16),
            pltpu.VMEM((R, hid), BF16),
            pltpu.VMEM((2, 2, R, blk), BF16),
            pltpu.VMEM((2, 2, R, blk), BF16),
            pltpu.VMEM((2, R, blk), BF16),
            pltpu.VMEM((2, R, blk), BF16),
            pltpu.VMEM((R, blk), BF16),
            pltpu.VMEM((R, blk), BF16),
            pltpu.VMEM((2, R, blk), F32),
            pltpu.VMEM((R, blk), F32),
            pltpu.VMEM((2, R, blk), BF16),
            dma, dma((hid // GT,)), dma((4,)), dma((2,)),
            dma((2,)), dma((2,)), dma, dma, dma, dma,
            dma((7, nc)), dma((7, nc)), dma((2,)), dma((nc,)),
            reg((2,)), reg, reg, reg((3,)),
        ],
        compiler_params=pltpu.CompilerParams(
            collective_id=0, has_side_effects=True, vmem_limit_bytes=67_043_328 - 2 * rows * d
        ),
        cost_estimate=pl.CostEstimate(
            flops=6 * rows * d * hid, bytes_accessed=2 * (12 * d * hid), transcendentals=rows * hid
        ),
        name="mlp_all_reduce",
    )(x, wg, wu, wd)[0]


def solution(mesh):
    return jax.shard_map(
        block,
        mesh=mesh,
        in_specs=(P("dp", None), P(None, "tp"), P(None, "tp"), P("tp", None)),
        out_specs=P("dp", None),
        check_vma=False,
    )
```
